256 devices in a mesh: trial: 4 (over z_lo), lat: 2 (over z_hi), lon: 4 (over x_hi, core), lev: 8 (over y, x_lo).
Axes of the slice: x: 4 (x_hi: 2, x_lo: 2; x = x_hi * 2 + x_lo), y: 4, z: 8 (z_hi: 2, z_lo: 4; z = z_hi * 4 + z_lo), core: 2. Of those that a mesh axis runs over, the one named last changes fastest.
Arguments:
- density: float32 [32, 64, 1024, 128], P(('trial', 'lat'), 'lon', 'lev'), parts along dimension 0, may hold values from 0.5 to 2
- crowding: float32 [32, 64, 1024, 128], P(('trial', 'lat'), 'lon', 'lev'), parts along dimension 0, may hold values from 0.5 to 2
Outputs:
- scaled_field: float32 [32, 64, 1024, 128], P(('trial', 'lat'), 'lon', 'lev'), parts along dimension 0
- density_end: float32 [32, 64, 1024, 128], P(('trial', 'lat'), 'lon', 'lev'), parts along dimension 0
The draws below stay inside these ranges and needn't reach their ends.
There are 4 independent parts, one for each index of `trial`. The reference program is written for one: setup_inputs(seed, part) draws one part's arguments, and reference() takes and returns one part's arrays. A program takes and returns all parts, laid end to end along the dimension named above; each array names one. Nothing has to cross between parts.
All inputs are finite; a program needn't handle non-finite values.
Results may differ from the reference program's by a relative error of at most 0.000058.
Values sent between devices are 32-bit elements; how exact they have to be, the bound alone decides.
A program may use at most 64 MiB of HBM per device.

```python
import jax
import jax.numpy as jnp
from jax import lax

GRID_Y = 8
GRID_X = 64
GRID_Z = 1024
SPECIES = 128
STEPS = 4


def shard_levels(stream_key, extent, cuts, least, largest):
    level, own = 1.0, jax.random.fold_in(stream_key, 6)
    for dim, blocks in cuts:
        draws = jnp.exp(jax.random.uniform(jax.random.fold_in(own, dim), (blocks,), jnp.float32, least / len(cuts), largest / len(cuts)))
        level = level * jnp.repeat(draws, extent[dim] // blocks).reshape([-1 if axis == dim else 1 for axis in range(len(extent))])
    return level


def setup_inputs(seed: int = 0, part: int = 0) -> dict:
    arg_keys = jax.random.split(jax.random.key(seed), 3)
    own_keys = jax.random.split(jax.random.fold_in(arg_keys[2], part), 3)
    density = jnp.clip(0.5 + 1.5 * jax.random.uniform(own_keys[0], (GRID_Y, GRID_X, GRID_Z, SPECIES), jnp.float32) ** shard_levels(own_keys[0], (GRID_Y, GRID_X, GRID_Z, SPECIES), ((0, 2), (1, 4), (2, 8)), -0.2, 0.2), 0.5, 2.0)
    crowding = jnp.clip(0.5 + 1.5 * jax.random.uniform(own_keys[1], (GRID_Y, GRID_X, GRID_Z, SPECIES), jnp.float32) ** shard_levels(own_keys[1], (GRID_Y, GRID_X, GRID_Z, SPECIES), ((0, 2), (1, 4), (2, 8)), -0.2, 0.2), 0.5, 2.0)
    return dict(density=density, crowding=crowding)


def inner_cells(values, dims):
    for dim in dims:
        values = lax.slice_in_dim(values, 1, values.shape[dim] - 1, axis=dim)
    return values

def side_cells(values, dim, start, dims):
    others = [other for other in dims if other != dim]
    values = inner_cells(values, others)
    return lax.slice_in_dim(values, start, start + values.shape[dim] - 2, axis=dim)

def advance(padded, crowding):
    middle = inner_cells(padded, (0, 1, 2))
    lower = [side_cells(padded, dim, 0, (0, 1, 2)) for dim in (0, 1, 2)]
    upper = [side_cells(padded, dim, 2, (0, 1, 2)) for dim in (0, 1, 2)]
    spread = lower[0] + upper[0] + lower[1] + upper[1] + lower[2] + upper[2] - 6.0 * middle
    return middle + 0.1 * spread + 0.2 * middle * (1.0 - middle * crowding)

def reference(density, crowding):
    for step in range(STEPS):
        density = advance(jnp.pad(density, ((1, 1), (1, 1), (1, 1), (0, 0)), mode='constant'), crowding)
    line_mean = lax.optimization_barrier(jnp.mean(density, axis=1, keepdims=True))
    centred = density - line_mean
    line_variance = lax.optimization_barrier(jnp.mean(centred * centred, axis=1, keepdims=True))
    scaled_field = centred * lax.rsqrt(line_variance + 0.0001)
    return (scaled_field, density)
```

```python
import functools

import jax
import jax.numpy as jnp
from jax import lax
from jax.experimental import pallas as pl
from jax.experimental.pallas import tpu as pltpu
from jax.sharding import PartitionSpec as P

STEPS = 4
TILE = 8
MESH = pl.DeviceIdType.MESH


def kernel(
    devices, shape, density, crowding, scaled_out, density_out,
    field, crowd, beyond, stats, load_sems,
    lat_send, lat_recv, lon_send, lon_recv, lev_send, lev_recv, stat_send, stat_recv,
):
    rows, wide, deep, _ = shape
    slabs = deep // TILE
    lat, lon, lev = (lax.axis_index(a) for a in ("lat", "lon", "lev"))
    lons, levs = devices["lon"], devices["lev"]

    def own_row(row):
        return lat * row + (1 - lat) * (rows - 1 - row)

    def slab_at(place):
        odd = place % 2
        return odd * (slabs - 1) + (1 - 2 * odd) * (place // 2)

    def inner(slab):
        return pl.ds(pl.multiple_of(slab * TILE, TILE), TILE)

    def padded(slab):
        return pl.ds(pl.multiple_of((slab + 1) * TILE, TILE), TILE)

    def lat_copy(parity, slab):
        return pltpu.make_async_remote_copy(
            src_ref=field.at[parity, 0, pl.ds(1, wide), padded(slab)],
            dst_ref=beyond.at[parity, :, inner(slab)],
            send_sem=lat_send.at[parity, slab],
            recv_sem=lat_recv.at[parity, slab],
            device_id={"lat": 1 - lat},
            device_id_type=MESH,
        )

    def lon_copy(parity, slab, up):
        return pltpu.make_async_remote_copy(
            src_ref=field.at[parity, :, wide if up else 1, padded(slab)],
            dst_ref=field.at[parity, :, 0 if up else wide + 1, padded(slab)],
            send_sem=lon_send.at[up, parity, slab],
            recv_sem=lon_recv.at[up, parity, slab],
            device_id={"lon": lon + (1 if up else -1)},
            device_id_type=MESH,
        )

    def lev_copy(parity, up):
        return pltpu.make_async_remote_copy(
            src_ref=field.at[parity, :, pl.ds(1, wide), pl.ds(deep if up else TILE, TILE)],
            dst_ref=field.at[parity, :, pl.ds(1, wide), pl.ds(0 if up else deep + TILE, TILE)],
            send_sem=lev_send.at[up, parity],
            recv_sem=lev_recv.at[up, parity],
            device_id={"lev": lev + (1 if up else -1)},
            device_id_type=MESH,
        )

    def stat_copy(slab, peer, source):
        return pltpu.make_async_remote_copy(
            src_ref=stats.at[slab, source],
            dst_ref=stats.at[slab, source],
            send_sem=stat_send.at[slab, peer],
            recv_sem=stat_recv.at[slab, source],
            device_id={"lon": peer},
            device_id_type=MESH,
        )

    def to_sides(slab, act):
        pl.when(lon > 0)(lambda: act(lambda parity: lon_copy(parity, slab, 0)))
        pl.when(lon < lons - 1)(lambda: act(lambda parity: lon_copy(parity, slab, 1)))
        pl.when((slab == 0) & (lev > 0))(lambda: act(lambda parity: lev_copy(parity, 0)))
        pl.when((slab == slabs - 1) & (lev < levs - 1))(lambda: act(lambda parity: lev_copy(parity, 1)))

    def from_sides(slab, act):
        pl.when(lon < lons - 1)(lambda: act(lambda parity: lon_copy(parity, slab, 0)))
        pl.when(lon > 0)(lambda: act(lambda parity: lon_copy(parity, slab, 1)))
        pl.when((slab == slabs - 1) & (lev < levs - 1))(lambda: act(lambda parity: lev_copy(parity, 0)))
        pl.when((slab == 0) & (lev > 0))(lambda: act(lambda parity: lev_copy(parity, 1)))

    def send(parity, slab):
        lat_copy(parity, slab).start()
        to_sides(slab, lambda copy: copy(parity).start())

    def wait_sent(parity, slab):
        lat_copy(parity, slab).wait_send()
        to_sides(slab, lambda copy: copy(parity).wait_send())

    def wait_received(parity, slab):
        from_sides(slab, lambda copy: copy(parity).wait_recv())
        lat_copy(parity, slab).wait_recv()

    def after(parity, slab, row):
        xs = pl.ds(1, wide)
        start = pl.multiple_of((slab + 1) * TILE, TILE)
        middle = field[parity, row, xs, pl.ds(start, TILE)]
        around = field[parity, row, xs, pl.ds(start - 1, TILE)] + field[parity, row, xs, pl.ds(start + 1, TILE)]
        around += field[parity, row, pl.ds(0, wide), pl.ds(start, TILE)]
        around += field[parity, row, pl.ds(2, wide), pl.ds(start, TILE)]
        around += beyond[parity, :, inner(slab)] if row == 0 else field[parity, row - 1, xs, pl.ds(start, TILE)]
        if row < rows - 1:
            around += field[parity, row + 1, xs, pl.ds(start, TILE)]
        return middle * (0.6 - 0.2 * (middle * crowd[row, :, inner(slab)])) + 0.1 * around

    loads = []
    for row in range(rows):
        loads.append(
            pltpu.make_async_copy(
                density.at[own_row(row)],
                field.at[0, row, pl.ds(1, wide), pl.ds(TILE, deep)],
                load_sems.at[0, row],
            )
        )
    for row in range(rows):
        loads.append(pltpu.make_async_copy(crowding.at[own_row(row)], crowd.at[row], load_sems.at[1, row]))
    for load in loads:
        load.start()

    @pl.loop(0, rows)
    def _(row):
        for parity in range(2):
            for x in (0, wide + 1):
                field[parity, row, x] = jnp.zeros(field.shape[3:], jnp.float32)
            for z in (0, deep + TILE):
                field[parity, row, pl.ds(1, wide), pl.ds(z, TILE)] = jnp.zeros((wide, TILE, field.shape[4]), jnp.float32)

    barrier = pltpu.get_barrier_semaphore()

    def greet(there):
        pl.semaphore_signal(barrier, 1, device_id=there, device_id_type=MESH)

    greet({"lat": 1 - lat})
    for away in range(1, lons):
        greet({"lon": (lon + away) % lons})
    pl.when(lev > 0)(lambda: greet({"lev": lev - 1}))
    pl.when(lev < levs - 1)(lambda: greet({"lev": lev + 1}))
    pl.semaphore_wait(barrier, lons + jnp.minimum(lev, 1) + jnp.minimum(levs - 1 - lev, 1))

    for load in loads[:rows]:
        load.wait()

    @pl.loop(0, slabs)
    def _(place):
        send(0, slab_at(place))

    for load in loads[rows:]:
        load.wait()

    @pl.loop(0, (STEPS - 1) * slabs)
    def _(count):
        step, slab = count // slabs, slab_at(count % slabs)
        now, later = step % 2, (step + 1) % 2
        pl.when(step > 0)(lambda: wait_sent(later, slab))
        wait_received(now, slab)
        for row in range(rows):
            field[later, row, pl.ds(1, wide), padded(slab)] = after(now, slab, row)
        send(later, slab)

    last = (STEPS - 1) % 2
    total_wide = wide * lons

    def finish(slab):
        for away in range(1, lons):
            stat_copy(slab, lon, (lon + away) % lons).wait_recv()
        sums = [stats[slab, source, 0] for source in range(lons)]
        squares = [stats[slab, source, 1] for source in range(lons)]
        mean = sum(sums) * (1.0 / total_wide)
        spread = sum(squares)
        for part in sums:
            apart = part * (1.0 / wide) - mean
            spread += wide * (apart * apart)
        scale = lax.rsqrt(spread * (1.0 / total_wide) + 0.0001)
        for row in range(rows):
            value = density_out[own_row(row), :, inner(slab)]
            scaled_out[own_row(row), :, inner(slab)] = (value - mean[row][None]) * scale[row][None]

    lag = 2

    @pl.loop(0, slabs)
    def _(place):
        slab = slab_at(place)
        wait_received(last, slab)
        for row in range(rows):
            value = after(last, slab, row)
            density_out[own_row(row), :, inner(slab)] = value
            part = jnp.sum(value, axis=0)
            moved = value - (part * (1.0 / wide))[None]
            stats[slab, lon, 0, row] = part
            stats[slab, lon, 1, row] = jnp.sum(moved * moved, axis=0)
        for away in range(1, lons):
            stat_copy(slab, (lon + away) % lons, lon).start()
        pl.when(place >= lag)(lambda: finish(slab_at(place - lag)))

    for place in range(slabs - lag, slabs):
        finish(slab_at(place))

    @pl.loop(0, slabs)
    def _(slab):
        wait_sent(1 - last, slab)
        wait_sent(last, slab)
        for away in range(1, lons):
            stat_copy(slab, (lon + away) % lons, lon).wait_send()


def shards(density, crowding, *, devices):
    rows, wide, deep, species = density.shape
    slabs = deep // TILE
    dma = pltpu.SemaphoreType.DMA
    return pl.pallas_call(
        functools.partial(kernel, devices, density.shape),
        out_shape=[jax.ShapeDtypeStruct(density.shape, jnp.float32)] * 2,
        in_specs=[pl.BlockSpec(memory_space=pl.ANY)] * 2,
        out_specs=[pl.BlockSpec(memory_space=pltpu.VMEM)] * 2,
        scratch_shapes=[
            pltpu.VMEM((2, rows, wide + 2, deep + 2 * TILE, species), jnp.float32),
            pltpu.VMEM((rows, wide, deep, species), jnp.float32),
            pltpu.VMEM((2, wide, deep, species), jnp.float32),
            pltpu.VMEM((slabs, devices["lon"], 2, rows, TILE, species), jnp.float32),
            dma((2, rows)),
            dma((2, slabs)),
            dma((2, slabs)),
            dma((2, 2, slabs)),
            dma((2, 2, slabs)),
            dma((2, 2)),
            dma((2, 2)),
            dma((slabs, devices["lon"])),
            dma((slabs, devices["lon"])),
        ],
        compiler_params=pltpu.CompilerParams(
            collective_id=0, has_side_effects=True, vmem_limit_bytes=44 * 2**20
        ),
        name="growth",
    )(density, crowding)


def solution(mesh):
    placed = P(("trial", "lat"), "lon", "lev", None)
    return jax.shard_map(
        functools.partial(shards, devices=dict(mesh.shape)),
        mesh=mesh,
        in_specs=(placed, placed),
        out_specs=(placed, placed),
        check_vma=False,
    )
```

```python
import functools

import jax
import jax.numpy as jnp
from jax import lax
from jax.experimental import pallas as pl
from jax.experimental.pallas import tpu as pltpu
from jax.sharding import PartitionSpec as P

STEPS = 4
TILE = 8
AHEAD_A = 12
AHEAD_B = 12
BUNCH = 4
MESH = pl.DeviceIdType.MESH


def bunches_of_places(slabs):
    at, bunches = 0, []
    while slabs - at > 1:
        bunches.append((at, (slabs - at) // 2))
        at += (slabs - at) // 2
    return [*bunches, (at, 1)]


def kernel(
    devices, shape, density, crowding, scaled_out, density_out,
    field, crowd, beyond, stats, load_sems, ready,
    lat_send, lat_recv, lon_send, lon_recv, lev_send, lev_recv, stat_send, stat_recv,
):
    rows, wide, deep, _ = shape
    slabs = deep // TILE
    trial = lax.axis_index("trial")
    ahead = AHEAD_A - (AHEAD_A - AHEAD_B) * (trial // 2)
    half = slabs // 2
    lat, lon, lev = (lax.axis_index(a) for a in ("lat", "lon", "lev"))
    lons, levs = devices["lon"], devices["lev"]
    sides = lons - 1 + jnp.minimum(lev, 1) + jnp.minimum(levs - 1 - lev, 1)
    bunches = bunches_of_places(slabs)

    def own_row(row):
        return lat * row + (1 - lat) * (rows - 1 - row)

    def slab_at(place):
        bunch = place // BUNCH
        odd = bunch % 2
        return (odd * (slabs // BUNCH - 1) + (1 - 2 * odd) * (bunch // 2)) * BUNCH + place % BUNCH

    def inner(slab):
        return pl.ds(pl.multiple_of(slab * TILE, TILE), TILE)

    def padded(slab, number=1):
        return pl.ds(pl.multiple_of((slab + 1) * TILE, TILE), number * TILE)

    def lat_copy(count):
        place = count % slabs
        slab = slab_at(place)
        return pltpu.make_async_remote_copy(
            src_ref=field.at[count // slabs % 2, 0, pl.ds(1, wide), padded(slab)],
            dst_ref=beyond.at[count // slabs % 2, :, inner(slab)],
            send_sem=lat_send.at[place],
            recv_sem=lat_recv.at[count // slabs % 2, place],
            device_id={"lat": 1 - lat},
            device_id_type=MESH,
        )

    def lon_copy(parity, first, up):
        cells = padded(first, BUNCH)
        return pltpu.make_async_remote_copy(
            src_ref=field.at[parity, :, wide if up else 1, cells],
            dst_ref=field.at[parity, :, 0 if up else wide + 1, cells],
            send_sem=lon_send.at[up, parity, first // BUNCH],
            recv_sem=lon_recv.at[up, parity, first // BUNCH],
            device_id={"lon": lon + (1 if up else -1)},
            device_id_type=MESH,
        )

    def lev_copy(parity, up):
        return pltpu.make_async_remote_copy(
            src_ref=field.at[parity, :, pl.ds(1, wide), pl.ds(deep if up else TILE, TILE)],
            dst_ref=field.at[parity, :, pl.ds(1, wide), pl.ds(0 if up else deep + TILE, TILE)],
            send_sem=lev_send.at[up, parity],
            recv_sem=lev_recv.at[up, parity],
            device_id={"lev": lev + (1 if up else -1)},
            device_id_type=MESH,
        )

    def on_both_sides(place, act, out, at):
        slab = slab_at(place)
        first = slab - at
        turn = place % BUNCH == at
        pl.when(turn & (lon > 0))(lambda: act(lambda parity: lon_copy(parity, first, 0 if out else 1)))
        pl.when(turn & (lon < lons - 1))(lambda: act(lambda parity: lon_copy(parity, first, 1 if out else 0)))
        pl.when((slab == 0) & (lev > 0))(lambda: act(lambda parity: lev_copy(parity, 0 if out else 1)))
        pl.when((slab == slabs - 1) & (lev < levs - 1))(lambda: act(lambda parity: lev_copy(parity, 1 if out else 0)))

    def send_sides(parity, place):
        on_both_sides(place, lambda copy: copy(parity).start(), True, BUNCH - 1)

    def wait_sent_sides(parity, place):
        on_both_sides(place, lambda copy: copy(parity).wait_send(), True, 0)

    def wait_sides(parity, place):
        on_both_sides(place, lambda copy: copy(parity).wait_recv(), False, 0)

    def send_ahead(count):
        later = count + ahead

        def send():
            pl.when(later >= slabs)(lambda: lat_copy(later - slabs).wait_send())
            lat_copy(later).start()

        pl.when(later < STEPS * slabs)(send)

    def after(parity, slab, row):
        xs = pl.ds(1, wide)
        start = pl.multiple_of((slab + 1) * TILE, TILE)
        middle = field[parity, row, xs, pl.ds(start, TILE)]
        before = field[parity, row, xs, padded(slab - 1)]
        behind = field[parity, row, xs, padded(slab + 1)]
        z = lax.broadcasted_iota(jnp.int32, middle.shape, 1)
        around = pltpu.roll(jnp.where(z == TILE - 1, before, middle), 1, 1)
        around += pltpu.roll(jnp.where(z == 0, behind, middle), TILE - 1, 1)
        around += field[parity, row, pl.ds(0, wide), pl.ds(start, TILE)]
        around += field[parity, row, pl.ds(2, wide), pl.ds(start, TILE)]
        around += beyond[parity, :, inner(slab)] if row == 0 else field[parity, row - 1, xs, pl.ds(start, TILE)]
        if row < rows - 1:
            around += field[parity, row + 1, xs, pl.ds(start, TILE)]
        return middle * (0.6 - 0.2 * (middle * crowd[row, :, inner(slab)])) + 0.1 * around

    barrier = pltpu.get_barrier_semaphore()

    def tell(semaphore, there):
        pl.semaphore_signal(semaphore, 1, device_id=there, device_id_type=MESH)

    def tell_sides(semaphore):
        for away in range(1, lons):
            tell(semaphore, {"lon": (lon + away) % lons})
        pl.when(lev > 0)(lambda: tell(semaphore, {"lev": lev - 1}))
        pl.when(lev < levs - 1)(lambda: tell(semaphore, {"lev": lev + 1}))

    def load_field(row):
        into = field.at[0, row, pl.ds(1, wide), pl.ds(TILE, deep)]
        return pltpu.make_async_copy(density.at[own_row(row)], into, load_sems.at[min(row, 1)])

    def load_crowd(row):
        return pltpu.make_async_copy(crowding.at[own_row(row)], crowd.at[row], load_sems.at[2])

    load_field(0).start()
    tell(barrier, {"lat": 1 - lat})
    pl.when(lat == 0)(lambda: tell_sides(barrier))
    load_field(0).wait()
    for row in range(1, rows):
        load_field(row).start()
    for row in range(rows):
        load_crowd(row).start()
    pl.semaphore_wait(barrier, 1 + (1 - lat) * sides)

    @pl.loop(0, ahead)
    def _(count):
        send_ahead(count - ahead)

    pl.when(lat == 0)(lambda: tell_sides(ready))

    def clear(row, x, z):
        for parity in range(2):
            field[parity, row, x, z] = jnp.zeros_like(field[parity, row, x, z])

    @pl.loop(0, rows)
    def _(row):
        pl.when(lon == 0)(lambda: clear(row, pl.ds(0, 1), pl.ds(0, deep + 2 * TILE)))
        pl.when(lon == lons - 1)(lambda: clear(row, pl.ds(wide + 1, 1), pl.ds(0, deep + 2 * TILE)))
        pl.when(lev == 0)(lambda: clear(row, pl.ds(1, wide), pl.ds(0, TILE)))
        pl.when(lev == levs - 1)(lambda: clear(row, pl.ds(1, wide), pl.ds(deep + TILE, TILE)))

    pl.semaphore_wait(ready, lat + (1 - lat) * sides)
    pl.when(lat == 0)(lambda: tell(ready, {"lat": 1}))
    others = pl.ds(1, rows - 1)
    pltpu.make_async_copy(
        density.at[others], field.at[0, others, pl.ds(1, wide), pl.ds(TILE, deep)], load_sems.at[1]
    ).wait()

    @pl.loop(0, slabs)
    def _(place):
        send_sides(0, place)

    pltpu.make_async_copy(crowding, crowd, load_sems.at[2]).wait()

    @pl.loop(0, (STEPS - 1) * slabs)
    def _(count):
        step, place = count // slabs, count % slabs
        slab = slab_at(place)
        now, later = step % 2, (step + 1) % 2
        pl.when(step > 0)(lambda: wait_sent_sides(later, place))
        wait_sides(now, place)
        lat_copy(count).wait_recv()
        for row in range(rows):
            field[later, row, pl.ds(1, wide), padded(slab)] = after(now, slab, row)
        send_sides(later, place)
        send_ahead(count)

    last = (STEPS - 1) % 2
    total_wide = wide * lons

    def stat_copy(sem, first, number, near, peer):
        part = stats.at[pl.ds(first, number), lon, pl.ds(0, 1) if near else pl.ds(1, rows - 1)]
        return pltpu.make_async_remote_copy(
            src_ref=part,
            dst_ref=part,
            send_sem=stat_send.at[0],
            recv_sem=stat_recv.at[sem],
            device_id={"lon": peer},
            device_id_type=MESH,
        )

    def send_stats(sem, first, number, near):
        for away in range(1, lons):
            stat_copy(sem, first, number, near, (lon + away) % lons).start()

    def wait_stats(sem, first, number, near):
        part = stats.at[pl.ds(first, number), pl.ds(0, lons - 1), pl.ds(0, 1) if near else pl.ds(1, rows - 1)]
        pltpu.make_async_remote_copy(
            src_ref=part,
            dst_ref=part,
            send_sem=stat_send.at[0],
            recv_sem=stat_recv.at[sem],
            device_id={"lon": lon},
            device_id_type=MESH,
        ).wait_recv()

    def close(row, place):
        slab = slab_at(place)
        value = after(last, slab, row)
        density_out[own_row(row), :, inner(slab)] = value
        part = jnp.sum(value, axis=0)
        moved = value - (part * (1.0 / wide))[None]
        stats[place, lon, row, 0] = part
        stats[place, lon, row, 1] = jnp.sum(moved * moved, axis=0)

    def finish(row, place):
        slab = slab_at(place)
        sums = [stats[place, source, row, 0] for source in range(lons)]
        mean = sum(sums) * (1.0 / total_wide)
        spread = sum(stats[place, source, row, 1] for source in range(lons))
        for part in sums:
            apart = part * (1.0 / wide) - mean
            spread += wide * (apart * apart)
        scale = lax.rsqrt(spread * (1.0 / total_wide) + 0.0001)
        value = density_out[own_row(row), :, inner(slab)]
        scaled_out[own_row(row), :, inner(slab)] = (value - mean[None]) * scale[None]

    @pl.loop(0, slabs)
    def _(place):
        wait_sides(last, place)
        for row in range(1, rows):
            close(row, place)
        for part in range(2):
            pl.when(place == (part + 1) * half - 1)(lambda: send_stats(part, part * half, half, False))

    @pl.loop(0, slabs)
    def _(place):
        lat_copy((STEPS - 1) * slabs + place).wait_recv()
        close(0, place)
        for which, (first, number) in enumerate(bunches):
            pl.when(place == first + number - 1)(lambda: send_stats(2 + which, first, number, True))
        send_ahead((STEPS - 1) * slabs + place)
        for part in range(2):
            pl.when(place == half + part * half // 2)(lambda: wait_stats(part, part * half, half, False))

        @pl.when(place >= half)
        def _():
            for more in range(2):
                for row in range(1, rows):
                    finish(row, 2 * (place - half) + more)

        pl.when(place == slabs - half // 2)(lambda: wait_stats(2, *bunches[0], True))

        @pl.when(place >= slabs - half // 2)
        def _():
            for more in range(2):
                finish(0, 2 * (place - slabs + half // 2) + more)

    @pl.loop(0, slabs)
    def _(place):
        wait_sent_sides(1 - last, place)
        wait_sent_sides(last, place)
        lat_copy((STEPS - 1) * slabs + place).wait_send()

    for which, (first, number) in enumerate(bunches):
        if which > 0:
            wait_stats(2 + which, first, number, True)

            @pl.loop(first, first + number)
            def _(place):
                finish(0, place)

    part = stats.at[:, pl.ds(0, lons - 1)]
    pltpu.make_async_remote_copy(
        src_ref=part,
        dst_ref=part,
        send_sem=stat_send.at[0],
        recv_sem=stat_recv.at[0],
        device_id={"lon": lon},
        device_id_type=MESH,
    ).wait_send()


def shards(density, crowding, *, devices):
    rows, wide, deep, species = density.shape
    slabs = deep // TILE
    dma = pltpu.SemaphoreType.DMA
    return pl.pallas_call(
        functools.partial(kernel, devices, density.shape),
        out_shape=[jax.ShapeDtypeStruct(density.shape, jnp.float32)] * 2,
        in_specs=[pl.BlockSpec(memory_space=pl.ANY)] * 2,
        out_specs=[pl.BlockSpec(memory_space=pltpu.VMEM)] * 2,
        scratch_shapes=[
            pltpu.VMEM((2, rows, wide + 2, deep + 2 * TILE, species), jnp.float32),
            pltpu.VMEM((rows, wide, deep, species), jnp.float32),
            pltpu.VMEM((2, wide, deep, species), jnp.float32),
            pltpu.VMEM((slabs, devices["lon"], rows, 2, TILE, species), jnp.float32),
            dma((3,)),
            pltpu.SemaphoreType.REGULAR,
            dma((slabs,)),
            dma((2, slabs)),
            dma((2, 2, slabs // BUNCH)),
            dma((2, 2, slabs // BUNCH)),
            dma((2, 2)),
            dma((2, 2)),
            dma((1,)),
            dma((2 + len(bunches_of_places(slabs)),)),
        ],
        compiler_params=pltpu.CompilerParams(
            collective_id=0, has_side_effects=True, vmem_limit_bytes=44 * 2**20
        ),
        name="growth",
    )(density, crowding)


def solution(mesh):
    placed = P(("trial", "lat"), "lon", "lev", None)
    return jax.shard_map(
        functools.partial(shards, devices=dict(mesh.shape)),
        mesh=mesh,
        in_specs=(placed, placed),
        out_specs=(placed, placed),
        check_vma=False,
    )
```

```python
import functools

import jax
import jax.numpy as jnp
from jax import lax
from jax.experimental import pallas as pl
from jax.experimental.pallas import tpu as pltpu
from jax.sharding import PartitionSpec as P

STEPS = 4
TILE = 8
AHEAD_A = 12
AHEAD_B = 12
BUNCH = 4
MESH = pl.DeviceIdType.MESH


def bunches_of_places(slabs):
    at, bunches = 0, []
    while slabs - at > 1:
        bunches.append((at, (slabs - at) // 2))
        at += (slabs - at) // 2
    return [*bunches, (at, 1)]


def kernel(
    devices, shape, density, crowding, scaled_out, density_out,
    field, crowd, beyond, stats, load_sems, ready,
    lat_send, lat_recv, lon_send, lon_recv, lev_send, lev_recv, stat_send, stat_recv,
):
    rows, wide, deep, _ = shape
    slabs = deep // TILE
    trial = lax.axis_index("trial")
    ahead = AHEAD_A - (AHEAD_A - AHEAD_B) * (trial // 2)
    half = slabs // 2
    lat, lon, lev = (lax.axis_index(a) for a in ("lat", "lon", "lev"))
    lons, levs = devices["lon"], devices["lev"]
    sides = lons - 1 + jnp.minimum(lev, 1) + jnp.minimum(levs - 1 - lev, 1)
    bunches = bunches_of_places(slabs)

    def own_row(row):
        return lat * row + (1 - lat) * (rows - 1 - row)

    def slab_at(place):
        bunch = place // BUNCH
        odd = bunch % 2
        return (odd * (slabs // BUNCH - 1) + (1 - 2 * odd) * (bunch // 2)) * BUNCH + place % BUNCH

    def inner(slab):
        return pl.ds(pl.multiple_of(slab * TILE, TILE), TILE)

    def padded(slab, number=1):
        return pl.ds(pl.multiple_of((slab + 1) * TILE, TILE), number * TILE)

    def lat_copy(count):
        place = count % slabs
        slab = slab_at(place)
        return pltpu.make_async_remote_copy(
            src_ref=field.at[count // slabs % 2, 0, pl.ds(1, wide), padded(slab)],
            dst_ref=beyond.at[count // slabs % 2, :, inner(slab)],
            send_sem=lat_send.at[place],
            recv_sem=lat_recv.at[count // slabs % 2, place],
            device_id={"lat": 1 - lat},
            device_id_type=MESH,
        )

    def lon_copy(parity, first, up):
        cells = padded(first, BUNCH)
        return pltpu.make_async_remote_copy(
            src_ref=field.at[parity, :, wide if up else 1, cells],
            dst_ref=field.at[parity, :, 0 if up else wide + 1, cells],
            send_sem=lon_send.at[up, parity, first // BUNCH],
            recv_sem=lon_recv.at[up, parity, first // BUNCH],
            device_id={"lon": lon + (1 if up else -1)},
            device_id_type=MESH,
        )

    def lev_copy(parity, up):
        return pltpu.make_async_remote_copy(
            src_ref=field.at[parity, :, pl.ds(1, wide), pl.ds(deep + TILE - 1 if up else TILE, 1)],
            dst_ref=field.at[parity, :, pl.ds(1, wide), pl.ds(TILE - 1 if up else deep + TILE, 1)],
            send_sem=lev_send.at[up, parity],
            recv_sem=lev_recv.at[up, parity],
            device_id={"lev": lev + (1 if up else -1)},
            device_id_type=MESH,
        )

    def on_both_sides(place, act, out, at):
        slab = slab_at(place)
        first = slab - at
        turn = place % BUNCH == at
        pl.when(turn & (lon > 0))(lambda: act(lambda parity: lon_copy(parity, first, 0 if out else 1)))
        pl.when(turn & (lon < lons - 1))(lambda: act(lambda parity: lon_copy(parity, first, 1 if out else 0)))
        pl.when((slab == 0) & (lev > 0))(lambda: act(lambda parity: lev_copy(parity, 0 if out else 1)))
        pl.when((slab == slabs - 1) & (lev < levs - 1))(lambda: act(lambda parity: lev_copy(parity, 1 if out else 0)))

    def send_sides(parity, place):
        on_both_sides(place, lambda copy: copy(parity).start(), True, BUNCH - 1)

    def wait_sent_sides(parity, place):
        on_both_sides(place, lambda copy: copy(parity).wait_send(), True, 0)

    def wait_sides(parity, place):
        on_both_sides(place, lambda copy: copy(parity).wait_recv(), False, 0)

    def send_ahead(count):
        later = count + ahead

        def send():
            pl.when(later >= slabs)(lambda: lat_copy(later - slabs).wait_send())
            lat_copy(later).start()

        pl.when(later < STEPS * slabs)(send)

    def after(parity, slab, row):
        xs = pl.ds(1, wide)
        start = pl.multiple_of((slab + 1) * TILE, TILE)
        middle = field[parity, row, xs, pl.ds(start, TILE)]
        before = field[parity, row, xs, padded(slab - 1)]
        behind = field[parity, row, xs, padded(slab + 1)]
        z = lax.broadcasted_iota(jnp.int32, middle.shape, 1)
        around = pltpu.roll(jnp.where(z == TILE - 1, before, middle), 1, 1)
        around += pltpu.roll(jnp.where(z == 0, behind, middle), TILE - 1, 1)
        around += field[parity, row, pl.ds(0, wide), pl.ds(start, TILE)]
        around += field[parity, row, pl.ds(2, wide), pl.ds(start, TILE)]
        around += beyond[parity, :, inner(slab)] if row == 0 else field[parity, row - 1, xs, pl.ds(start, TILE)]
        if row < rows - 1:
            around += field[parity, row + 1, xs, pl.ds(start, TILE)]
        return middle * (0.6 - 0.2 * (middle * crowd[row, :, inner(slab)])) + 0.1 * around

    barrier = pltpu.get_barrier_semaphore()

    def tell(semaphore, there):
        pl.semaphore_signal(semaphore, 1, device_id=there, device_id_type=MESH)

    def tell_sides(semaphore):
        for away in range(1, lons):
            tell(semaphore, {"lon": (lon + away) % lons})
        pl.when(lev > 0)(lambda: tell(semaphore, {"lev": lev - 1}))
        pl.when(lev < levs - 1)(lambda: tell(semaphore, {"lev": lev + 1}))

    def load_field(row):
        into = field.at[0, row, pl.ds(1, wide), pl.ds(TILE, deep)]
        return pltpu.make_async_copy(density.at[own_row(row)], into, load_sems.at[min(row, 1)])

    def load_crowd(row):
        return pltpu.make_async_copy(crowding.at[own_row(row)], crowd.at[row], load_sems.at[2])

    load_field(0).start()
    tell(barrier, {"lat": 1 - lat})
    pl.when(lat == 0)(lambda: tell_sides(barrier))
    load_field(0).wait()
    for row in range(1, rows):
        load_field(row).start()
    for row in range(rows):
        load_crowd(row).start()
    pl.semaphore_wait(barrier, 1 + (1 - lat) * sides)

    @pl.loop(0, ahead)
    def _(count):
        send_ahead(count - ahead)

    pl.when(lat == 0)(lambda: tell_sides(ready))

    def clear(row, x, z):
        for parity in range(2):
            field[parity, row, x, z] = jnp.zeros_like(field[parity, row, x, z])

    @pl.loop(0, rows)
    def _(row):
        pl.when(lon == 0)(lambda: clear(row, pl.ds(0, 1), pl.ds(0, deep + 2 * TILE)))
        pl.when(lon == lons - 1)(lambda: clear(row, pl.ds(wide + 1, 1), pl.ds(0, deep + 2 * TILE)))
        pl.when(lev == 0)(lambda: clear(row, pl.ds(1, wide), pl.ds(0, TILE)))
        pl.when(lev == levs - 1)(lambda: clear(row, pl.ds(1, wide), pl.ds(deep + TILE, TILE)))

    pl.semaphore_wait(ready, lat + (1 - lat) * sides)
    pl.when(lat == 0)(lambda: tell(ready, {"lat": 1}))
    others = pl.ds(1, rows - 1)
    pltpu.make_async_copy(
        density.at[others], field.at[0, others, pl.ds(1, wide), pl.ds(TILE, deep)], load_sems.at[1]
    ).wait()

    @pl.loop(0, slabs)
    def _(place):
        send_sides(0, place)

    pltpu.make_async_copy(crowding, crowd, load_sems.at[2]).wait()

    @pl.loop(0, (STEPS - 1) * slabs)
    def _(count):
        step, place = count // slabs, count % slabs
        slab = slab_at(place)
        now, later = step % 2, (step + 1) % 2
        pl.when(step > 0)(lambda: wait_sent_sides(later, place))
        wait_sides(now, place)
        lat_copy(count).wait_recv()
        for row in range(rows):
            field[later, row, pl.ds(1, wide), padded(slab)] = after(now, slab, row)
        send_sides(later, place)
        send_ahead(count)

    last = (STEPS - 1) % 2
    total_wide = wide * lons

    def stat_copy(sem, first, number, near, peer):
        part = stats.at[pl.ds(first, number), lon, pl.ds(0, 1) if near else pl.ds(1, rows - 1)]
        return pltpu.make_async_remote_copy(
            src_ref=part,
            dst_ref=part,
            send_sem=stat_send.at[0],
            recv_sem=stat_recv.at[sem],
            device_id={"lon": peer},
            device_id_type=MESH,
        )

    def send_stats(sem, first, number, near):
        for away in range(1, lons):
            stat_copy(sem, first, number, near, (lon + away) % lons).start()

    def wait_stats(sem, first, number, near):
        part = stats.at[pl.ds(first, number), pl.ds(0, lons - 1), pl.ds(0, 1) if near else pl.ds(1, rows - 1)]
        pltpu.make_async_remote_copy(
            src_ref=part,
            dst_ref=part,
            send_sem=stat_send.at[0],
            recv_sem=stat_recv.at[sem],
            device_id={"lon": lon},
            device_id_type=MESH,
        ).wait_recv()

    def close(row, place):
        slab = slab_at(place)
        value = after(last, slab, row)
        density_out[own_row(row), :, inner(slab)] = value
        part = jnp.sum(value, axis=0)
        moved = value - (part * (1.0 / wide))[None]
        stats[place, lon, row, 0] = part
        stats[place, lon, row, 1] = jnp.sum(moved * moved, axis=0)

    def finish(row, place):
        slab = slab_at(place)
        sums = [stats[place, source, row, 0] for source in range(lons)]
        mean = sum(sums) * (1.0 / total_wide)
        spread = sum(stats[place, source, row, 1] for source in range(lons))
        for part in sums:
            apart = part * (1.0 / wide) - mean
            spread += wide * (apart * apart)
        scale = lax.rsqrt(spread * (1.0 / total_wide) + 0.0001)
        value = density_out[own_row(row), :, inner(slab)]
        scaled_out[own_row(row), :, inner(slab)] = (value - mean[None]) * scale[None]

    @pl.loop(0, slabs)
    def _(place):
        wait_sides(last, place)
        for row in range(1, rows):
            close(row, place)
        for part in range(2):
            pl.when(place == (part + 1) * half - 1)(lambda: send_stats(part, part * half, half, False))

    @pl.loop(0, slabs)
    def _(place):
        lat_copy((STEPS - 1) * slabs + place).wait_recv()
        close(0, place)
        for which, (first, number) in enumerate(bunches):
            pl.when(place == first + number - 1)(lambda: send_stats(2 + which, first, number, True))
        send_ahead((STEPS - 1) * slabs + place)
        for part in range(2):
            pl.when(place == half + part * half // 2)(lambda: wait_stats(part, part * half, half, False))

        @pl.when(place >= half)
        def _():
            for more in range(2):
                for row in range(1, rows):
                    finish(row, 2 * (place - half) + more)

        pl.when(place == slabs - half // 2)(lambda: wait_stats(2, *bunches[0], True))

        @pl.when(place >= slabs - half // 2)
        def _():
            for more in range(2):
                finish(0, 2 * (place - slabs + half // 2) + more)

    @pl.loop(0, slabs)
    def _(place):
        wait_sent_sides(1 - last, place)
        wait_sent_sides(last, place)
        lat_copy((STEPS - 1) * slabs + place).wait_send()

    for which, (first, number) in enumerate(bunches):
        if which > 0:
            wait_stats(2 + which, first, number, True)

            @pl.loop(first, first + number)
            def _(place):
                finish(0, place)

    part = stats.at[:, pl.ds(0, lons - 1)]
    pltpu.make_async_remote_copy(
        src_ref=part,
        dst_ref=part,
        send_sem=stat_send.at[0],
        recv_sem=stat_recv.at[0],
        device_id={"lon": lon},
        device_id_type=MESH,
    ).wait_send()


def deliver(scaled, density, scaled_out, density_out, sems):
    copies = []
    for part, (held, out) in enumerate(((scaled, scaled_out), (density, density_out))):
        for row in range(held.shape[0]):
            copies.append(pltpu.make_async_copy(held.at[row], out.at[row], sems.at[part, row]))
    for copy in copies:
        copy.start()
    for copy in copies:
        copy.wait()


def shards(density, crowding, *, devices):
    rows, wide, deep, species = density.shape
    slabs = deep // TILE
    dma = pltpu.SemaphoreType.DMA
    held = pl.pallas_call(
        functools.partial(kernel, devices, density.shape),
        out_shape=[jax.ShapeDtypeStruct(density.shape, jnp.float32)] * 2,
        in_specs=[pl.BlockSpec(memory_space=pl.ANY)] * 2,
        out_specs=[pl.BlockSpec(memory_space=pltpu.VMEM)] * 2,
        scratch_shapes=[
            pltpu.VMEM((2, rows, wide + 2, deep + 2 * TILE, species), jnp.float32),
            pltpu.VMEM((rows, wide, deep, species), jnp.float32),
            pltpu.VMEM((2, wide, deep, species), jnp.float32),
            pltpu.VMEM((slabs, devices["lon"], rows, 2, TILE, species), jnp.float32),
            dma((3,)),
            pltpu.SemaphoreType.REGULAR,
            dma((slabs,)),
            dma((2, slabs)),
            dma((2, 2, slabs // BUNCH)),
            dma((2, 2, slabs // BUNCH)),
            dma((2, 2)),
            dma((2, 2)),
            dma((1,)),
            dma((2 + len(bunches_of_places(slabs)),)),
        ],
        compiler_params=pltpu.CompilerParams(
            collective_id=0, has_side_effects=True, vmem_limit_bytes=44 * 2**20
        ),
        name="growth",
    )(density, crowding)
    return pl.pallas_call(
        deliver,
        out_shape=[jax.ShapeDtypeStruct(density.shape, jnp.float32)] * 2,
        in_specs=[pl.BlockSpec(memory_space=pltpu.VMEM)] * 2,
        out_specs=[pl.BlockSpec(memory_space=pl.ANY)] * 2,
        scratch_shapes=[dma((2, rows))],
        compiler_params=pltpu.CompilerParams(vmem_limit_bytes=44 * 2**20),
        name="deliver",
    )(*held)


def solution(mesh):
    placed = P(("trial", "lat"), "lon", "lev", None)
    return jax.shard_map(
        functools.partial(shards, devices=dict(mesh.shape)),
        mesh=mesh,
        in_specs=(placed, placed),
        out_specs=(placed, placed),
        check_vma=False,
    )
```

```python
import functools

import jax
import jax.numpy as jnp
from jax import lax
from jax.experimental import pallas as pl
from jax.experimental.pallas import tpu as pltpu
from jax.sharding import PartitionSpec as P

STEPS = 4
TILE = 8
AHEAD_A = 12
AHEAD_B = 12
BUNCH = 4
MESH = pl.DeviceIdType.MESH


def bunches_of_places(slabs):
    at, bunches = 0, []
    while slabs - at > 1:
        bunches.append((at, (slabs - at) // 2))
        at += (slabs - at) // 2
    return [*bunches, (at, 1)]


def kernel(
    devices, shape, density, crowding, scaled_out, density_out,
    field, crowd, beyond, stats, load_sems, ready,
    lat_send, lat_recv, lon_send, lon_recv, lev_send, lev_recv, stat_send, stat_recv,
):
    rows, wide, deep, _ = shape
    slabs = deep // TILE
    trial = lax.axis_index("trial")
    ahead = AHEAD_A - (AHEAD_A - AHEAD_B) * (trial // 2)
    half = slabs // 2
    lat, lon, lev = (lax.axis_index(a) for a in ("lat", "lon", "lev"))
    lons, levs = devices["lon"], devices["lev"]
    sides = lons - 1 + jnp.minimum(lev, 1) + jnp.minimum(levs - 1 - lev, 1)
    bunches = bunches_of_places(slabs)

    def own_row(row):
        return lat * row + (1 - lat) * (rows - 1 - row)

    def slab_at(place):
        bunch = place // BUNCH
        odd = bunch % 2
        return (odd * (slabs // BUNCH - 1) + (1 - 2 * odd) * (bunch // 2)) * BUNCH + place % BUNCH

    def inner(slab, number=1):
        return pl.ds(pl.multiple_of(slab * TILE, TILE), number * TILE)

    def padded(slab, number=1):
        return pl.ds(pl.multiple_of((slab + 1) * TILE, TILE), number * TILE)

    def lat_copy(count, number=1):
        place = count % slabs
        slab = slab_at(place)
        return pltpu.make_async_remote_copy(
            src_ref=field.at[count // slabs % 2, 0, pl.ds(1, wide), padded(slab, number)],
            dst_ref=beyond.at[count // slabs % 2, :, inner(slab, number)],
            send_sem=lat_send.at[place // BUNCH],
            recv_sem=lat_recv.at[count // slabs % 2, place],
            device_id={"lat": 1 - lat},
            device_id_type=MESH,
        )

    def lon_copy(parity, first, up):
        cells = padded(first, BUNCH)
        return pltpu.make_async_remote_copy(
            src_ref=field.at[parity, :, wide if up else 1, cells],
            dst_ref=field.at[parity, :, 0 if up else wide + 1, cells],
            send_sem=lon_send.at[up, parity, first // BUNCH],
            recv_sem=lon_recv.at[up, parity, first // BUNCH],
            device_id={"lon": lon + (1 if up else -1)},
            device_id_type=MESH,
        )

    def lev_copy(parity, up):
        return pltpu.make_async_remote_copy(
            src_ref=field.at[parity, :, pl.ds(1, wide), pl.ds(deep + TILE - 1 if up else TILE, 1)],
            dst_ref=field.at[parity, :, pl.ds(1, wide), pl.ds(TILE - 1 if up else deep + TILE, 1)],
            send_sem=lev_send.at[up, parity],
            recv_sem=lev_recv.at[up, parity],
            device_id={"lev": lev + (1 if up else -1)},
            device_id_type=MESH,
        )

    def on_both_sides(place, act, out, at):
        slab = slab_at(place)
        first = slab - at
        turn = place % BUNCH == at
        pl.when(turn & (lon > 0))(lambda: act(lambda parity: lon_copy(parity, first, 0 if out else 1)))
        pl.when(turn & (lon < lons - 1))(lambda: act(lambda parity: lon_copy(parity, first, 1 if out else 0)))
        pl.when((slab == 0) & (lev > 0))(lambda: act(lambda parity: lev_copy(parity, 0 if out else 1)))
        pl.when((slab == slabs - 1) & (lev < levs - 1))(lambda: act(lambda parity: lev_copy(parity, 1 if out else 0)))

    def send_sides(parity, place):
        on_both_sides(place, lambda copy: copy(parity).start(), True, BUNCH - 1)

    def wait_sent_sides(parity, place):
        on_both_sides(place, lambda copy: copy(parity).wait_send(), True, 0)

    def wait_sides(parity, place):
        on_both_sides(place, lambda copy: copy(parity).wait_recv(), False, 0)

    def send_ahead(count):
        later = count + ahead

        def send():
            turn = (later >= slabs) & (later % BUNCH == 0)
            pl.when(turn)(lambda: lat_copy(later - slabs, BUNCH).wait_send())
            lat_copy(later).start()

        pl.when(later < STEPS * slabs)(send)

    def after(parity, slab, row):
        xs = pl.ds(1, wide)
        start = pl.multiple_of((slab + 1) * TILE, TILE)
        middle = field[parity, row, xs, pl.ds(start, TILE)]
        before = field[parity, row, xs, padded(slab - 1)]
        behind = field[parity, row, xs, padded(slab + 1)]
        z = lax.broadcasted_iota(jnp.int32, middle.shape, 1)
        around = pltpu.roll(jnp.where(z == TILE - 1, before, middle), 1, 1)
        around += pltpu.roll(jnp.where(z == 0, behind, middle), TILE - 1, 1)
        around += field[parity, row, pl.ds(0, wide), pl.ds(start, TILE)]
        around += field[parity, row, pl.ds(2, wide), pl.ds(start, TILE)]
        around += beyond[parity, :, inner(slab)] if row == 0 else field[parity, row - 1, xs, pl.ds(start, TILE)]
        if row < rows - 1:
            around += field[parity, row + 1, xs, pl.ds(start, TILE)]
        return middle * (0.6 - 0.2 * (middle * crowd[row, :, inner(slab)])) + 0.1 * around

    barrier = pltpu.get_barrier_semaphore()

    def tell(semaphore, there):
        pl.semaphore_signal(semaphore, 1, device_id=there, device_id_type=MESH)

    def tell_sides(semaphore):
        for away in range(1, lons):
            tell(semaphore, {"lon": (lon + away) % lons})
        pl.when(lev > 0)(lambda: tell(semaphore, {"lev": lev - 1}))
        pl.when(lev < levs - 1)(lambda: tell(semaphore, {"lev": lev + 1}))

    def load_field(row):
        into = field.at[0, row, pl.ds(1, wide), pl.ds(TILE, deep)]
        return pltpu.make_async_copy(density.at[own_row(row)], into, load_sems.at[min(row, 1)])

    def load_crowd(row):
        return pltpu.make_async_copy(crowding.at[own_row(row)], crowd.at[row], load_sems.at[2])

    load_field(0).start()
    tell(barrier, {"lat": 1 - lat})
    pl.when(lat == 0)(lambda: tell_sides(barrier))
    load_field(0).wait()
    for row in range(1, rows):
        load_field(row).start()
    for row in range(rows):
        load_crowd(row).start()
    pl.semaphore_wait(barrier, 1 + (1 - lat) * sides)

    @pl.loop(0, ahead)
    def _(count):
        send_ahead(count - ahead)

    pl.when(lat == 0)(lambda: tell_sides(ready))

    def clear(row, x, z):
        for parity in range(2):
            field[parity, row, x, z] = jnp.zeros_like(field[parity, row, x, z])

    @pl.loop(0, rows)
    def _(row):
        pl.when(lon == 0)(lambda: clear(row, pl.ds(0, 1), pl.ds(0, deep + 2 * TILE)))
        pl.when(lon == lons - 1)(lambda: clear(row, pl.ds(wide + 1, 1), pl.ds(0, deep + 2 * TILE)))
        pl.when(lev == 0)(lambda: clear(row, pl.ds(1, wide), pl.ds(0, TILE)))
        pl.when(lev == levs - 1)(lambda: clear(row, pl.ds(1, wide), pl.ds(deep + TILE, TILE)))

    pl.semaphore_wait(ready, lat + (1 - lat) * sides)
    pl.when(lat == 0)(lambda: tell(ready, {"lat": 1}))
    others = pl.ds(1, rows - 1)
    pltpu.make_async_copy(
        density.at[others], field.at[0, others, pl.ds(1, wide), pl.ds(TILE, deep)], load_sems.at[1]
    ).wait()

    @pl.loop(0, slabs)
    def _(place):
        send_sides(0, place)

    pltpu.make_async_copy(crowding, crowd, load_sems.at[2]).wait()

    @pl.loop(0, (STEPS - 1) * slabs)
    def _(count):
        step, place = count // slabs, count % slabs
        slab = slab_at(place)
        now, later = step % 2, (step + 1) % 2
        pl.when(step > 0)(lambda: wait_sent_sides(later, place))
        wait_sides(now, place)
        lat_copy(count).wait_recv()
        for row in range(rows):
            field[later, row, pl.ds(1, wide), padded(slab)] = after(now, slab, row)
        send_sides(later, place)
        send_ahead(count)

    last = (STEPS - 1) % 2
    total_wide = wide * lons

    def stat_copy(sem, first, number, near, peer):
        part = stats.at[pl.ds(first, number), lon, pl.ds(0, 1) if near else pl.ds(1, rows - 1)]
        return pltpu.make_async_remote_copy(
            src_ref=part,
            dst_ref=part,
            send_sem=stat_send.at[0],
            recv_sem=stat_recv.at[sem],
            device_id={"lon": peer},
            device_id_type=MESH,
        )

    def send_stats(sem, first, number, near):
        for away in range(1, lons):
            stat_copy(sem, first, number, near, (lon + away) % lons).start()

    def wait_stats(sem, first, number, near):
        part = stats.at[pl.ds(first, number), pl.ds(0, lons - 1), pl.ds(0, 1) if near else pl.ds(1, rows - 1)]
        pltpu.make_async_remote_copy(
            src_ref=part,
            dst_ref=part,
            send_sem=stat_send.at[0],
            recv_sem=stat_recv.at[sem],
            device_id={"lon": lon},
            device_id_type=MESH,
        ).wait_recv()

    def close(row, place):
        slab = slab_at(place)
        value = after(last, slab, row)
        density_out[own_row(row), :, inner(slab)] = value
        part = jnp.sum(value, axis=0)
        moved = value - (part * (1.0 / wide))[None]
        stats[place, lon, row, 0] = part
        stats[place, lon, row, 1] = jnp.sum(moved * moved, axis=0)

    def finish(row, place):
        slab = slab_at(place)
        sums = [stats[place, source, row, 0] for source in range(lons)]
        mean = sum(sums) * (1.0 / total_wide)
        spread = sum(stats[place, source, row, 1] for source in range(lons))
        for part in sums:
            apart = part * (1.0 / wide) - mean
            spread += wide * (apart * apart)
        scale = lax.rsqrt(spread * (1.0 / total_wide) + 0.0001)
        value = density_out[own_row(row), :, inner(slab)]
        scaled_out[own_row(row), :, inner(slab)] = (value - mean[None]) * scale[None]

    @pl.loop(0, slabs)
    def _(place):
        wait_sides(last, place)
        for row in range(1, rows):
            close(row, place)
        for part in range(2):
            pl.when(place == (part + 1) * half - 1)(lambda: send_stats(part, part * half, half, False))

    @pl.loop(0, slabs)
    def _(place):
        lat_copy((STEPS - 1) * slabs + place).wait_recv()
        close(0, place)
        for which, (first, number) in enumerate(bunches):
            pl.when(place == first + number - 1)(lambda: send_stats(2 + which, first, number, True))
        send_ahead((STEPS - 1) * slabs + place)
        for part in range(2):
            pl.when(place == half + part * half // 2)(lambda: wait_stats(part, part * half, half, False))

        @pl.when(place >= half)
        def _():
            for more in range(2):
                for row in range(1, rows):
                    finish(row, 2 * (place - half) + more)

        pl.when(place == slabs - half // 2)(lambda: wait_stats(2, *bunches[0], True))

        @pl.when(place >= slabs - half // 2)
        def _():
            for more in range(2):
                finish(0, 2 * (place - slabs + half // 2) + more)

    @pl.loop(0, slabs)
    def _(place):
        wait_sent_sides(1 - last, place)
        wait_sent_sides(last, place)
        turn = place % BUNCH == 0
        pl.when(turn)(lambda: lat_copy((STEPS - 1) * slabs + place, BUNCH).wait_send())

    for which, (first, number) in enumerate(bunches):
        if which > 0:
            wait_stats(2 + which, first, number, True)

            @pl.loop(first, first + number)
            def _(place):
                finish(0, place)

    part = stats.at[:, pl.ds(0, lons - 1)]
    pltpu.make_async_remote_copy(
        src_ref=part,
        dst_ref=part,
        send_sem=stat_send.at[0],
        recv_sem=stat_recv.at[0],
        device_id={"lon": lon},
        device_id_type=MESH,
    ).wait_send()


def deliver(scaled, density, scaled_out, density_out, sems):
    copies = []
    for part, (held, out) in enumerate(((scaled, scaled_out), (density, density_out))):
        for row in range(held.shape[0]):
            copies.append(pltpu.make_async_copy(held.at[row], out.at[row], sems.at[part, row]))
    for copy in copies:
        copy.start()
    for copy in copies:
        copy.wait()


def shards(density, crowding, *, devices):
    rows, wide, deep, species = density.shape
    slabs = deep // TILE
    dma = pltpu.SemaphoreType.DMA
    held = pl.pallas_call(
        functools.partial(kernel, devices, density.shape),
        out_shape=[jax.ShapeDtypeStruct(density.shape, jnp.float32)] * 2,
        in_specs=[pl.BlockSpec(memory_space=pl.ANY)] * 2,
        out_specs=[pl.BlockSpec(memory_space=pltpu.VMEM)] * 2,
        scratch_shapes=[
            pltpu.VMEM((2, rows, wide + 2, deep + 2 * TILE, species), jnp.float32),
            pltpu.VMEM((rows, wide, deep, species), jnp.float32),
            pltpu.VMEM((2, wide, deep, species), jnp.float32),
            pltpu.VMEM((slabs, devices["lon"], rows, 2, TILE, species), jnp.float32),
            dma((3,)),
            pltpu.SemaphoreType.REGULAR,
            dma((slabs // BUNCH,)),
            dma((2, slabs)),
            dma((2, 2, slabs // BUNCH)),
            dma((2, 2, slabs // BUNCH)),
            dma((2, 2)),
            dma((2, 2)),
            dma((1,)),
            dma((2 + len(bunches_of_places(slabs)),)),
        ],
        compiler_params=pltpu.CompilerParams(
            collective_id=0, has_side_effects=True, vmem_limit_bytes=44 * 2**20
        ),
        name="growth",
    )(density, crowding)
    return pl.pallas_call(
        deliver,
        out_shape=[jax.ShapeDtypeStruct(density.shape, jnp.float32)] * 2,
        in_specs=[pl.BlockSpec(memory_space=pltpu.VMEM)] * 2,
        out_specs=[pl.BlockSpec(memory_space=pl.ANY)] * 2,
        scratch_shapes=[dma((2, rows))],
        compiler_params=pltpu.CompilerParams(vmem_limit_bytes=44 * 2**20),
        name="deliver",
    )(*held)


def solution(mesh):
    placed = P(("trial", "lat"), "lon", "lev", None)
    return jax.shard_map(
        functools.partial(shards, devices=dict(mesh.shape)),
        mesh=mesh,
        in_specs=(placed, placed),
        out_specs=(placed, placed),
        check_vma=False,
    )
```
